8 devices in a mesh: fsdp: 8 (over z, y, x, core).
Axes of the slice: x: 2, y: 2, z: 1, core: 2. Of those that a mesh axis runs over, the one named last changes fastest.
Arguments:
- patches: bfloat16 [64, 196, 768], P('fsdp')
- keep: int32 [64, 98], P('fsdp')
- w_patch: float32 [768, 384], P(None, 'fsdp')
- b_patch: float32 [384], P('fsdp')
- pos_table: float32 [197, 384], P(None, 'fsdp')
- cls_tok: float32 [384], P('fsdp')
- lnp_g: float32 [384], P('fsdp')
- lnp_b: float32 [384], P('fsdp')
- ln1_g: float32 [384], P('fsdp')
- ln1_b: float32 [384], P('fsdp')
- w_qkv: float32 [384, 3, 6, 64], P('fsdp')
- b_qkv: float32 [1152], P('fsdp')
- w_out: float32 [384, 384], P('fsdp')
- b_out: float32 [384], P('fsdp')
- ln2_g: float32 [384], P('fsdp')
- ln2_b: float32 [384], P('fsdp')
- w_fc: float32 [384, 1536], P('fsdp')
- b_fc: float32 [1536], P('fsdp')
- w_proj: float32 [1536, 384], P('fsdp')
- b_proj: float32 [384], P('fsdp')
- grad_h1: bfloat16 [64, 99, 384], P('fsdp')
Outputs:
- output 1: bfloat16 [64, 99, 384], P('fsdp')
- output 2: float32 [768, 384], P(None, 'fsdp')
- output 3: float32 [384], P('fsdp')
- output 4: float32 [197, 384], P(None, 'fsdp')
- output 5: float32 [384], P('fsdp')
- output 6: float32 [384], P('fsdp')
- output 7: float32 [384], P('fsdp')
- output 8: float32 [384], P('fsdp')
- output 9: float32 [384], P('fsdp')
- output 10: float32 [384, 3, 6, 64], P('fsdp')
- output 11: float32 [1152], P('fsdp')
- output 12: float32 [384, 384], P('fsdp')
- output 13: float32 [384], P('fsdp')
- output 14: float32 [384], P('fsdp')
- output 15: float32 [384], P('fsdp')
- output 16: float32 [384, 1536], P('fsdp')
- output 17: float32 [1536], P('fsdp')
- output 18: float32 [1536, 384], P('fsdp')
- output 19: float32 [384], P('fsdp')
All inputs are finite; a program needn't handle non-finite values.
Results may differ from the reference program's by a relative error of at most 0.02.
Values are sent between devices in bfloat16 or wider.
A program may use at most 1 GiB of HBM per device.

```python
import jax
import jax.numpy as jnp
from jax import lax

MODEL_WIDTH = 384
NUM_HEADS = 6
MLP_WIDTH = 1536
NUM_PATCHES = 196
PATCH_PIXELS = 768
NUM_KEEP = 98
BATCH_SIZE = 64
BLOCK_IMAGES = 8
TOKENS = NUM_KEEP + 1
HEAD_DIM = MODEL_WIDTH // NUM_HEADS
LN_EPS = 1e-5
INV_SQRT2 = 0.7071067811865476
INV_SQRT_2PI = 0.3989422804014327
PARAM_NAMES = ('w_patch', 'b_patch', 'pos_table', 'cls_tok', 'lnp_g', 'lnp_b', 'ln1_g', 'ln1_b', 'w_qkv', 'b_qkv', 'w_out', 'b_out', 'ln2_g', 'ln2_b', 'w_fc', 'b_fc', 'w_proj', 'b_proj')
VECTOR_NAMES = ('b_patch', 'cls_tok', 'lnp_g', 'lnp_b', 'ln1_g', 'ln1_b', 'b_qkv', 'b_out', 'ln2_g', 'ln2_b', 'b_fc', 'b_proj')


def setup_inputs(seed: int = 0) -> dict:
    key_list = jax.random.split(jax.random.key(seed), 21)
    d_model = MODEL_WIDTH
    mlp_width = MLP_WIDTH

    def draw_normal(index, shape, scale):
        return jax.random.normal(key_list[index], shape, jnp.float32) * scale

    def gain_vec(index):
        return 1.0 + draw_normal(index, (d_model,), 0.2)

    row_keys = jax.random.split(key_list[1], BATCH_SIZE)
    perm_rows = jax.vmap(lambda row_key: jax.random.permutation(row_key, NUM_PATCHES))(row_keys)
    return {
        'patches': draw_normal(0, (BATCH_SIZE, NUM_PATCHES, PATCH_PIXELS), 1.0).astype(jnp.bfloat16),
        'keep': perm_rows[:, :NUM_KEEP].astype(jnp.int32),
        'w_patch': draw_normal(2, (PATCH_PIXELS, d_model), PATCH_PIXELS ** -0.5),
        'b_patch': draw_normal(3, (d_model,), 0.3),
        'pos_table': draw_normal(4, (NUM_PATCHES + 1, d_model), 0.5),
        'cls_tok': draw_normal(5, (d_model,), 1.0),
        'lnp_g': gain_vec(6),
        'lnp_b': draw_normal(7, (d_model,), 0.2),
        'ln1_g': gain_vec(8),
        'ln1_b': draw_normal(9, (d_model,), 0.2),
        'w_qkv': draw_normal(10, (d_model, 3, NUM_HEADS, HEAD_DIM), d_model ** -0.5),
        'b_qkv': draw_normal(11, (3 * d_model,), 0.3),
        'w_out': draw_normal(12, (d_model, d_model), d_model ** -0.5),
        'b_out': draw_normal(13, (d_model,), 0.3),
        'ln2_g': gain_vec(14),
        'ln2_b': draw_normal(15, (d_model,), 0.2),
        'w_fc': draw_normal(16, (d_model, mlp_width), d_model ** -0.5),
        'b_fc': draw_normal(17, (mlp_width,), 0.3),
        'w_proj': draw_normal(18, (mlp_width, d_model), mlp_width ** -0.5),
        'b_proj': draw_normal(19, (d_model,), 0.3),
        'grad_h1': draw_normal(20, (BATCH_SIZE, TOKENS, d_model), (BATCH_SIZE * TOKENS) ** -0.5).astype(jnp.bfloat16),
    }


def product(einsum_form, left_op, right_op):
    return jnp.einsum(einsum_form, left_op.astype(jnp.float32), right_op.astype(jnp.float32))


def norm_forward(x_in, gain_f, shift_f):
    centered = x_in - jnp.mean(x_in, axis=-1, keepdims=True)
    inv_std = lax.rsqrt(jnp.mean(centered * centered, axis=-1, keepdims=True) + LN_EPS)
    x_hat = centered * inv_std
    return x_hat * gain_f + shift_f, x_hat, inv_std


def norm_backward(d_norm, x_hat, inv_std, gain_f):
    d_hat = d_norm * gain_f
    d_in = inv_std * (d_hat - jnp.mean(d_hat, axis=-1, keepdims=True) - x_hat * jnp.mean(d_hat * x_hat, axis=-1, keepdims=True))
    return d_in, jnp.sum(d_norm * x_hat, axis=(0, 1)), jnp.sum(d_norm, axis=(0, 1))


def gelu_slope(pre_act):
    return 0.5 * (1.0 + lax.erf(pre_act * INV_SQRT2)) + pre_act * jnp.exp(-0.5 * pre_act * pre_act) * INV_SQRT_2PI


def forward(full_w, patches, keep):
    n_img = patches.shape[0]
    d_model = full_w['w_out'].shape[0]
    n_heads, head_dim = full_w['w_qkv'].shape[2], full_w['w_qkv'].shape[3]
    logit_scale = head_dim ** -0.5
    as_f32 = {name: full_w[name].astype(jnp.float32) for name in VECTOR_NAMES}
    kept_rows = jnp.take_along_axis(patches, keep[:, :, None], axis=1)
    embed_rows = product('bkq,qw->bkw', kept_rows, full_w['w_patch']) + as_f32['b_patch'] + full_w['pos_table'][1 + keep].astype(jnp.float32)
    head_row = as_f32['cls_tok'] + full_w['pos_table'][0].astype(jnp.float32)
    x_zero = jnp.concatenate([jnp.broadcast_to(head_row, (n_img, 1, d_model)), embed_rows], axis=1)
    h_zero, hat_p, inv_p = norm_forward(x_zero, as_f32['lnp_g'], as_f32['lnp_b'])
    y_one, hat_1, inv_1 = norm_forward(h_zero, as_f32['ln1_g'], as_f32['ln1_b'])
    a_in = y_one.astype(jnp.bfloat16)
    qkv_all = (product('btw,wchd->btchd', a_in, full_w['w_qkv']) + as_f32['b_qkv'].reshape(3, n_heads, head_dim)).astype(jnp.bfloat16)
    q_heads, k_heads, v_heads = qkv_all[:, :, 0], qkv_all[:, :, 1], qkv_all[:, :, 2]
    attn_prob = jax.nn.softmax(product('bqhd,bkhd->bhqk', q_heads, k_heads) * logit_scale, axis=-1)
    prob_b = attn_prob.astype(jnp.bfloat16)
    context = product('bhqk,bkhd->bqhd', prob_b, v_heads).astype(jnp.bfloat16)
    h_mid = h_zero + product('bqhd,hdw->bqw', context, full_w['w_out'].reshape(n_heads, head_dim, d_model)) + as_f32['b_out']
    y_two, hat_2, inv_2 = norm_forward(h_mid, as_f32['ln2_g'], as_f32['ln2_b'])
    c_in = y_two.astype(jnp.bfloat16)
    pre_act = product('btw,wf->btf', c_in, full_w['w_fc']) + as_f32['b_fc']
    gelu_out = jax.nn.gelu(pre_act, approximate=False).astype(jnp.bfloat16)
    h_one = (h_mid + product('btf,fw->btw', gelu_out, full_w['w_proj']) + as_f32['b_proj']).astype(jnp.bfloat16)
    saved = dict(keep=keep, kept_rows=kept_rows, hat_p=hat_p, inv_p=inv_p, hat_1=hat_1, inv_1=inv_1, a_in=a_in, q_heads=q_heads, k_heads=k_heads, v_heads=v_heads, attn_prob=attn_prob, prob_b=prob_b, context=context, hat_2=hat_2, inv_2=inv_2, c_in=c_in, pre_act=pre_act, gelu_out=gelu_out)
    return h_one, saved


def backward(weights, saved, grad_h1):
    d_model = weights['w_out'].shape[0]
    n_heads, head_dim = weights['w_qkv'].shape[2], weights['w_qkv'].shape[3]
    logit_scale = head_dim ** -0.5
    w_out3 = weights['w_out'].reshape(n_heads, head_dim, d_model)
    d_h = grad_h1.astype(jnp.float32)
    g_w_proj = product('btf,btw->fw', saved['gelu_out'], grad_h1)
    d_pre = product('btw,fw->btf', grad_h1, weights['w_proj']) * gelu_slope(saved['pre_act'])
    d_pre_b = d_pre.astype(jnp.bfloat16)
    g_w_fc = product('btw,btf->wf', saved['c_in'], d_pre_b)
    d_c = product('btf,wf->btw', d_pre_b, weights['w_fc'])
    d_norm2, g_ln2_g, g_ln2_b = norm_backward(d_c, saved['hat_2'], saved['inv_2'], weights['ln2_g'].astype(jnp.float32))
    d_mid = d_norm2 + d_h
    d_mid_b = d_mid.astype(jnp.bfloat16)
    g_w_out = product('bqhd,bqw->hdw', saved['context'], d_mid_b).reshape(d_model, d_model)
    d_ctx = product('bqw,hdw->bqhd', d_mid_b, w_out3).astype(jnp.bfloat16)
    g_v = product('bhqk,bqhd->bkhd', saved['prob_b'], d_ctx)
    d_prob = product('bqhd,bkhd->bhqk', d_ctx, saved['v_heads'])
    attn_prob = saved['attn_prob']
    d_logit = (attn_prob * (d_prob - jnp.sum(attn_prob * d_prob, axis=-1, keepdims=True)) * logit_scale).astype(jnp.bfloat16)
    g_q = product('bhqk,bkhd->bqhd', d_logit, saved['k_heads'])
    g_k = product('bhqk,bqhd->bkhd', d_logit, saved['q_heads'])
    d_qkv = jnp.stack([g_q, g_k, g_v], axis=2)
    d_qkv_b = d_qkv.astype(jnp.bfloat16)
    g_w_qkv = product('btw,btchd->wchd', saved['a_in'], d_qkv_b)
    d_a = product('btchd,wchd->btw', d_qkv_b, weights['w_qkv'])
    d_norm1, g_ln1_g, g_ln1_b = norm_backward(d_a, saved['hat_1'], saved['inv_1'], weights['ln1_g'].astype(jnp.float32))
    d_zero = d_norm1 + d_mid
    d_x, g_lnp_g, g_lnp_b = norm_backward(d_zero, saved['hat_p'], saved['inv_p'], weights['lnp_g'].astype(jnp.float32))
    d_head = jnp.sum(d_x[:, 0], axis=0)
    d_emb = d_x[:, 1:]
    d_emb_b = d_emb.astype(jnp.bfloat16)
    pos_rest = jax.ops.segment_sum(d_emb_b.astype(jnp.float32).reshape(-1, d_model), saved['keep'].reshape(-1), num_segments=NUM_PATCHES)
    g_pos = jnp.concatenate([d_head[None], pos_rest], axis=0)
    return dict(w_patch=product('bkq,bkw->qw', saved['kept_rows'], d_emb_b), b_patch=jnp.sum(d_emb, axis=(0, 1)), pos_table=g_pos, cls_tok=d_head, lnp_g=g_lnp_g, lnp_b=g_lnp_b, ln1_g=g_ln1_g, ln1_b=g_ln1_b, w_qkv=g_w_qkv, b_qkv=jnp.sum(d_qkv, axis=(0, 1)).reshape(-1), w_out=g_w_out, b_out=jnp.sum(d_mid, axis=(0, 1)), ln2_g=g_ln2_g, ln2_b=g_ln2_b, w_fc=g_w_fc, b_fc=jnp.sum(d_pre, axis=(0, 1)), w_proj=g_w_proj, b_proj=jnp.sum(d_h, axis=(0, 1)))


def reference(patches, keep, w_patch, b_patch, pos_table, cls_tok, lnp_g, lnp_b, ln1_g, ln1_b, w_qkv, b_qkv, w_out, b_out, ln2_g, ln2_b, w_fc, b_fc, w_proj, b_proj, grad_h1):
    masters = (w_patch, b_patch, pos_table, cls_tok, lnp_g, lnp_b, ln1_g, ln1_b, w_qkv, b_qkv, w_out, b_out, ln2_g, ln2_b, w_fc, b_fc, w_proj, b_proj)
    full_w = {name: value.astype(jnp.bfloat16) for name, value in zip(PARAM_NAMES, masters)}
    n_blocks = BATCH_SIZE // BLOCK_IMAGES

    def split_blocks(array_in):
        return array_in.reshape((n_blocks, BLOCK_IMAGES) + array_in.shape[1:])

    def scan_step(running, block_in):
        h_one, saved = forward(full_w, block_in[0], block_in[1])
        grad_map = backward(full_w, saved, block_in[2])
        return {name: running[name] + grad_map[name] for name in PARAM_NAMES}, h_one

    zero_grads = {name: jnp.zeros(value.shape, jnp.float32) for name, value in zip(PARAM_NAMES, masters)}
    totals, h_blocks = lax.scan(scan_step, zero_grads, (split_blocks(patches), split_blocks(keep), split_blocks(grad_h1)))
    h_out = h_blocks.reshape(BATCH_SIZE, TOKENS, MODEL_WIDTH)
    return (h_out, totals['w_patch'], totals['b_patch'], totals['pos_table'], totals['cls_tok'], totals['lnp_g'], totals['lnp_b'], totals['ln1_g'], totals['ln1_b'], totals['w_qkv'], totals['b_qkv'], totals['w_out'], totals['b_out'], totals['ln2_g'], totals['ln2_b'], totals['w_fc'], totals['b_fc'], totals['w_proj'], totals['b_proj'])
```

```python
import functools

import jax
import jax.numpy as jnp
from jax import lax
from jax.experimental import pallas as pl
from jax.experimental.pallas import tpu as pltpu
from jax.sharding import PartitionSpec as P

AXIS = 'fsdp'
LN_EPS = 1e-5
INV_SQRT2 = 0.7071067811865476
INV_SQRT_2PI = 0.3989422804014327
PARAM_NAMES = ('w_patch', 'b_patch', 'pos_table', 'cls_tok', 'lnp_g', 'lnp_b', 'ln1_g', 'ln1_b', 'w_qkv', 'b_qkv', 'w_out', 'b_out', 'ln2_g', 'ln2_b', 'w_fc', 'b_fc', 'w_proj', 'b_proj')
VROWS = ('b_patch', 'cls_tok', 'lnp_g', 'lnp_b', 'ln1_g', 'ln1_b', 'b_out', 'ln2_g', 'ln2_b', 'b_proj', 'b_qkv', 'b_fc')
ROW = {name: i for i, name in enumerate(VROWS)}
LAST_SPLIT = ('w_patch', 'pos_table')
MESH = pl.DeviceIdType.MESH

NDEV = 8
IMG = 8
NPATCH = 196
NKEEP = 98
TOK = 99
TP = 112
NT = IMG * TP
D = 384
HD = 64
PAIRS = 3
FF = 1536
QKV3 = 1152
PX = 768
PPOS = 256
SUB = D // NDEV
SUBF = FF // NDEV
RB = 224
F32 = jnp.float32
BF16 = jnp.bfloat16


def dot(a, b):
    return jnp.dot(a, b, preferred_element_type=F32)


def dot_nt(a, b):
    return lax.dot_general(a, b, (((1,), (1,)), ((), ())), preferred_element_type=F32)


def dot_tn(a, b):
    return lax.dot_general(a, b, (((0,), (0,)), ((), ())), preferred_element_type=F32)


def norm_stats(x):
    mu = jnp.mean(x, axis=-1, keepdims=True)
    c = x - mu
    inv = lax.rsqrt(jnp.mean(c * c, axis=-1, keepdims=True) + LN_EPS)
    return c * inv, inv


def norm_back(d_norm, x_hat, inv, gain):
    d_hat = d_norm * gain
    m1 = jnp.mean(d_hat, axis=-1, keepdims=True)
    m2 = jnp.mean(d_hat * x_hat, axis=-1, keepdims=True)
    return inv * (d_hat - m1 - x_hat * m2)


def rows_sum(x):
    return jnp.sum(x, axis=0, keepdims=True)


MATS = (('wp', SUB, PX), ('pt', SUB, PPOS), ('qkv', SUB, QKV3), ('out', SUB, D), ('fc', SUB, FF), ('proj', SUBF, D))
NMAT = len(MATS)
VEC = NMAT


def step_kernel(patches, keep, gh_in, w_patch, pos, w_qkv, w_out, w_fc, w_proj, *rest):
    vec_in = rest[:12]
    (h1_out, o_wp, o_pt, o_qkv, o_out, o_fc, o_proj, o_vec) = rest[12:20]
    (kb, z_s, oh_s, wwp, wpt, wqkv, wout, wfc, wproj, vg, v384, vqkv, vfc,
     hat_p, hat_1, hat_2, inv_p, inv_1, inv_2, h_s, a_s, qkv_s, p_s, ctx_s, c_s, gel_s, dpre_s, gh_s, dmid_s, dmb_s, dctx_s, dqkv_s, deb_s,
     gv384, gvqkv, gvfc) = rest[20:56]
    grads = rest[56:63]
    sibs = rest[63:70]
    rds = rest[70:77]
    rss = rest[77:84]
    rfs = rest[84:91]
    g_send, g_recv, r_send, r_recv = rest[91:95]
    outs = (o_wp, o_pt, o_qkv, o_out, o_fc, o_proj, o_vec)

    me = lax.axis_index(AXIS)
    core = lax.rem(me, 2)
    chip = me // 2
    xi = lax.rem(chip, 2)
    yi = chip // 2
    dx = 2 - 4 * xi
    dy = 4 - 8 * yi
    sib = me + 1 - 2 * core
    first = me + dx + core * (dy - dx)
    second = me + dy + core * (dx - dy)
    diag = me + dx + dy

    weights = (wwp, wpt, wqkv, wout, wfc, wproj)
    eye = (lax.broadcasted_iota(jnp.int32, (SUB, SUB), 0) == lax.broadcasted_iota(jnp.int32, (SUB, SUB), 1)).astype(BF16)

    def piece(k, slot):
        if k == VEC:
            return vg.at[slot]
        rows = MATS[k][1]
        return weights[k].at[pl.ds(pl.multiple_of(slot * rows, 16), rows), :]

    def own(k):
        rows = MATS[k][1]
        return pl.ds(pl.multiple_of(me * rows, 16), rows)

    vrow = jnp.zeros((16, 256), F32)
    vg[pl.ds(me, 1)] = vrow.reshape(1, 16, 256)
    for i, ref in enumerate(vec_in):
        width = ref.shape[1]
        vg[pl.ds(me, 1), i:i + 1, 0:width] = ref[...].astype(BF16).astype(F32).reshape(1, 1, width)
    wwp[own(0), :] = dot_nt(eye, w_patch[...].astype(BF16)).astype(BF16)
    wpt[own(1), :] = jnp.zeros((SUB, PPOS), BF16)
    wpt[own(1), 0:NPATCH + 1] = dot_nt(eye, pos[...].astype(BF16)).astype(BF16)
    wqkv[own(2), :] = w_qkv[...].astype(BF16)
    wout[own(3), :] = w_out[...].astype(BF16)
    wfc[own(4), :] = w_fc[...].astype(BF16)
    wproj[own(5), :] = w_proj[...].astype(BF16)

    barrier = pltpu.get_barrier_semaphore()
    for peer in (sib, first, second):
        pl.semaphore_signal(barrier, inc=1, device_id=(peer,), device_id_type=MESH)
    pl.semaphore_wait(barrier, 3)

    def gcopy(k, kind):
        slot, dev = ((me, first), (me, second), (first, second), (me, sib), (first, sib), (second, sib), (diag, sib))[kind]
        return pltpu.make_async_remote_copy(src_ref=piece(k, slot), dst_ref=piece(k, slot), send_sem=g_send.at[k * 7 + kind],
                                            recv_sem=g_recv.at[k * 7 + kind], device_id=(dev,), device_id_type=MESH)

    def gather_start(k):
        gcopy(k, 0).start()
        gcopy(k, 1).start()
        gcopy(k, 3).start()

    def gather_near(k):
        gcopy(k, 0).wait_recv()
        gcopy(k, 2).start()
        gcopy(k, 4).start()
        gcopy(k, 1).wait_recv()
        gcopy(k, 5).start()

    def gather_far(k):
        gcopy(k, 2).wait_recv()
        gcopy(k, 6).start()

    def gather_done(k):
        for kind in (3, 4, 5, 6):
            gcopy(k, kind).wait_recv()

    for k in (0, 1, VEC, 2, 3, 4, 5):
        gather_start(k)

    schip = second // 2
    fchip = first // 2
    dchip = diag // 2

    def rcopy(k, kind):
        g = grads[k]
        src, dst, dev = ((g.at[:, 1 - core], sibs[k], sib), (g.at[dchip, core], rds[k], second),
                         (g.at[schip, core], rss[k], second), (g.at[fchip, core], rfs[k], first))[kind]
        return pltpu.make_async_remote_copy(src_ref=src, dst_ref=dst, send_sem=r_send.at[k * 4 + kind],
                                            recv_sem=r_recv.at[k * 4 + kind], device_id=(dev,), device_id_type=MESH)

    def add_sib(k, c):
        grads[k][c, core] = grads[k][c, core] + sibs[k][c]

    def rs_a(k):
        rcopy(k, 0).start()

    def rs_b(k):
        rcopy(k, 0).wait_recv()
        add_sib(k, dchip)
        add_sib(k, schip)
        rcopy(k, 1).start()
        rcopy(k, 2).start()
        add_sib(k, fchip)
        add_sib(k, chip)

    def rs_c(k):
        rcopy(k, 1).wait_recv()
        grads[k][fchip, core] = grads[k][fchip, core] + rds[k][...]
        rcopy(k, 3).start()

    def rs_d(k):
        rcopy(k, 2).wait_recv()
        rcopy(k, 3).wait_recv()
        outs[k][...] = grads[k][chip, core] + rss[k][...] + rfs[k][...]

    def put(k, val, col=0):
        rows = MATS[k][1]
        width = val.shape[1]
        for o in range(val.shape[0] // rows):
            grads[k][o // 2, o % 2, :, col:col + width] = val[o * rows:(o + 1) * rows, :]

    kb[...] = jnp.full((IMG, 128), -1, jnp.int32)
    kb[:, 0:NKEEP] = keep[...]
    kb[...] = pltpu.roll(kb[...], 1, 1)
    lane = lax.broadcasted_iota(jnp.int32, (1, 128), 1)
    for i in range(IMG):
        kp = jnp.where(lane == 0, 0, kb[i:i + 1, :] + 1)
        kp = jnp.where(lane > NKEEP, -1, kp)
        oh_t = (lax.broadcasted_iota(jnp.int32, (PPOS, 128), 0) == kp).astype(F32)
        oh = oh_t.T[0:TP, :].astype(BF16)
        oh_s[i * TP:(i + 1) * TP, :] = oh
        oh_p = ((lax.broadcasted_iota(jnp.int32, (PPOS, 128), 0) + 1) == kp).astype(F32)
        ohp = oh_p.T[0:TP, 0:NPATCH].astype(BF16)
        z_s[i * TP:(i + 1) * TP, :] = dot(ohp, patches[i]).astype(BF16)
        gh_s[i * TP:(i + 1) * TP, :] = jnp.zeros((TP, D), BF16)
        gh_s[i * TP:i * TP + TOK, :] = gh_in[i]

    gv384[...] = jnp.zeros((16, D), F32)
    gvqkv[...] = jnp.zeros((8, QKV3), F32)
    gvfc[...] = jnp.zeros((8, FF), F32)

    for k in (0, 1, VEC):
        gather_near(k)
    for k in (0, 1, VEC):
        gather_far(k)
    for k in (0, 1, VEC):
        gather_done(k)

    acc_a = jnp.zeros((16, D), F32)
    acc_q = jnp.zeros((8, QKV3), F32)
    acc_f = jnp.zeros((8, FF), F32)
    for d in range(NDEV):
        x = vg[d]
        acc_a += pltpu.roll(jnp.concatenate([x[:, 0:128], jnp.zeros((16, D - 128), F32)], axis=1), SUB * d, 1)
        acc_q += pltpu.roll(jnp.concatenate([x[8:16, :], jnp.zeros((8, QKV3 - 256), F32)], axis=1), (QKV3 // NDEV) * d, 1)
        acc_f += pltpu.roll(jnp.concatenate([x[8:16, :], jnp.zeros((8, FF - 256), F32)], axis=1), SUBF * d, 1)
    v384[...] = acc_a
    vqkv[...] = acc_q
    vfc[...] = acc_f

    def vec(name):
        r = ROW[name]
        return v384[r:r + 1, :]

    def gacc(name, val):
        r = ROW[name]
        gv384[r:r + 1, :] = gv384[r:r + 1, :] + val

    def blocks(body, n=NT // RB, size=RB):
        def step(b, carry):
            body(pl.ds(pl.multiple_of(b * size, size), size))
            return carry
        lax.fori_loop(0, n, step, 0)

    tok_row = lax.rem(lax.broadcasted_iota(jnp.int32, (RB, 1), 0), TP)
    is_cls = tok_row == 0

    def embed(rs):
        e = dot_nt(z_s[rs, :], wwp[...]) + dot_nt(oh_s[rs, :], wpt[...])
        x0 = e + jnp.where(is_cls, vec('cls_tok'), vec('b_patch'))
        xh, inv = norm_stats(x0)
        h0 = xh * vec('lnp_g') + vec('lnp_b')
        hat_p[rs, :] = xh
        inv_p[rs, :] = inv
        h_s[rs, :] = h0
        xh1, inv1 = norm_stats(h0)
        hat_1[rs, :] = xh1
        inv_1[rs, :] = inv1
        a_s[rs, :] = (xh1 * vec('ln1_g') + vec('ln1_b')).astype(BF16)

    blocks(embed)
    gather_near(2)
    gather_far(2)
    gather_done(2)

    def qkv_body(rs):
        qkv_s[rs, :] = (dot(a_s[rs, :], wqkv[...]) + vqkv[2:3, :]).astype(BF16)

    blocks(qkv_body)
    gather_near(3)
    gather_near(4)
    gather_far(3)

    lane_b = lax.broadcasted_iota(jnp.int32, (1, 128), 1)
    lo = (lane_b < HD).astype(F32).astype(BF16)
    hi = (lane_b >= HD).astype(F32).astype(BF16)
    lo_mask = lane_b < HD
    key_ok = lax.broadcasted_iota(jnp.int32, (1, TP, 1), 1) < TOK
    scale = HD ** -0.5

    def att_fwd(i, carry):
        rs = pl.ds(pl.multiple_of(i * TP, TP), TP)
        for j in range(PAIRS):
            cs = slice(j * 128, (j + 1) * 128)
            q = qkv_s[rs, cs]
            k = qkv_s[rs, D + j * 128:D + (j + 1) * 128]
            v = qkv_s[rs, 2 * D + j * 128:2 * D + (j + 1) * 128]
            kk = jnp.concatenate([k * lo, k * hi], axis=0)
            vv = jnp.concatenate([v * lo, v * hi], axis=0)
            s = (dot_nt(kk, q) * scale).reshape(2, TP, TP)
            s = jnp.where(key_ok, s, -jnp.inf)
            e = jnp.exp(s - jnp.max(s, axis=1, keepdims=True))
            p = (e / jnp.sum(e, axis=1, keepdims=True)).reshape(2 * TP, TP)
            p_s[i * PAIRS + j] = p
            ctx_s[rs, cs] = dot_tn(p.astype(BF16), vv).astype(BF16)
        return carry

    lax.fori_loop(0, IMG, att_fwd, 0)
    gather_done(3)
    gather_far(4)
    gather_near(5)

    def out_body(rs):
        hm = h_s[rs, :] + dot(ctx_s[rs, :], wout[...]) + vec('b_out')
        h_s[rs, :] = hm
        xh, inv = norm_stats(hm)
        hat_2[rs, :] = xh
        inv_2[rs, :] = inv
        c_s[rs, :] = (xh * vec('ln2_g') + vec('ln2_b')).astype(BF16)

    blocks(out_body)
    gather_done(4)
    gather_far(5)
    gather_done(5)

    def mlp(rs):
        c = c_s[rs, :]
        gh = gh_s[rs, :]
        for j in range(FF // 512):
            cs = slice(j * 512, (j + 1) * 512)
            u = dot(c, wfc[:, cs]) + vfc[3:4, cs]
            cdf = 0.5 * (1.0 + lax.erf(u * INV_SQRT2))
            gel_s[rs, cs] = (u * cdf).astype(BF16)
            slope = cdf + u * jnp.exp(-0.5 * u * u) * INV_SQRT_2PI
            d_pre = dot_nt(gh, wproj[cs, :]) * slope
            dpre_s[rs, cs] = d_pre.astype(BF16)
            gvfc[3:4, cs] = gvfc[3:4, cs] + rows_sum(d_pre)

    blocks(mlp)

    PROJ, FC, OUT, QKV, WP, PT = 5, 4, 3, 2, 0, 1
    for j in range(FF // 384):
        put_val = dot_tn(gel_s[:, j * 384:(j + 1) * 384], gh_s[...])
        for o in range(2):
            d = j * 2 + o
            grads[PROJ][d // 2, d % 2, :, :] = put_val[o * SUBF:(o + 1) * SUBF, :]
    rs_a(PROJ)
    for j in range(FF // 384):
        put(FC, dot_tn(c_s[...], dpre_s[:, j * 384:(j + 1) * 384]), j * 384)
    rs_a(FC)
    rs_b(PROJ)

    def mid(rs):
        d_c = dot_nt(dpre_s[rs, :], wfc[...])
        xh = hat_2[rs, :]
        gacc('ln2_g', rows_sum(d_c * xh))
        gacc('ln2_b', rows_sum(d_c))
        d_h = gh_s[rs, :].astype(F32)
        gacc('b_proj', rows_sum(d_h))
        d_mid = norm_back(d_c, xh, inv_2[rs, :], vec('ln2_g')) + d_h
        gacc('b_out', rows_sum(d_mid))
        dmid_s[rs, :] = d_mid
        dmb = d_mid.astype(BF16)
        dmb_s[rs, :] = dmb
        dctx_s[rs, :] = dot_nt(dmb, wout[...]).astype(BF16)

    blocks(mid)
    rs_b(FC)
    rs_c(PROJ)
    put(OUT, dot_tn(ctx_s[...], dmb_s[...]))
    rs_a(OUT)

    def att_bwd(i, carry):
        rs = pl.ds(pl.multiple_of(i * TP, TP), TP)
        for j in range(PAIRS):
            cs = slice(j * 128, (j + 1) * 128)
            q = qkv_s[rs, cs]
            k = qkv_s[rs, D + j * 128:D + (j + 1) * 128]
            v = qkv_s[rs, 2 * D + j * 128:2 * D + (j + 1) * 128]
            kk = jnp.concatenate([k * lo, k * hi], axis=0)
            vv = jnp.concatenate([v * lo, v * hi], axis=0)
            dctx = dctx_s[rs, cs]
            p = p_s[i * PAIRS + j]
            dp = dot_nt(vv, dctx)
            t = jnp.sum((p * dp).reshape(2, TP, TP), axis=1, keepdims=True)
            dl = (p * (dp.reshape(2, TP, TP) - t).reshape(2 * TP, TP) * scale).astype(BF16)
            gv2 = dot(p.astype(BF16), dctx)
            gk2 = dot(dl, q)
            g_q = dot_tn(dl, kk)
            g_k = jnp.where(lo_mask, gk2[0:TP, :], gk2[TP:, :])
            g_v = jnp.where(lo_mask, gv2[0:TP, :], gv2[TP:, :])
            for s, g in ((0, g_q), (1, g_k), (2, g_v)):
                c0 = s * D + j * 128
                dqkv_s[rs, c0:c0 + 128] = g.astype(BF16)
                gvqkv[2:3, c0:c0 + 128] = gvqkv[2:3, c0:c0 + 128] + rows_sum(g)
        return carry

    lax.fori_loop(0, IMG // 2, att_bwd, 0)
    rs_b(OUT)
    rs_c(FC)
    lax.fori_loop(IMG // 2, IMG, att_bwd, 0)

    for j in range(3):
        put(QKV, dot_tn(a_s[...], dqkv_s[:, j * 384:(j + 1) * 384]), j * 384)
    rs_a(QKV)
    rs_c(OUT)
    rs_d(PROJ)

    def front(rs):
        d_a = dot_nt(dqkv_s[rs, :], wqkv[...])
        xh1 = hat_1[rs, :]
        gacc('ln1_g', rows_sum(d_a * xh1))
        gacc('ln1_b', rows_sum(d_a))
        d_zero = norm_back(d_a, xh1, inv_1[rs, :], vec('ln1_g')) + dmid_s[rs, :]
        xhp = hat_p[rs, :]
        gacc('lnp_g', rows_sum(d_zero * xhp))
        gacc('lnp_b', rows_sum(d_zero))
        d_x = norm_back(d_zero, xhp, inv_p[rs, :], vec('lnp_g'))
        gacc('cls_tok', rows_sum(jnp.where(is_cls, d_x, 0.0)))
        d_emb = jnp.where(is_cls, 0.0, d_x)
        gacc('b_patch', rows_sum(d_emb))
        deb_s[rs, :] = d_emb.astype(BF16)

    blocks(front)
    rs_b(QKV)
    for j in range(2):
        put(WP, dot_tn(deb_s[...], z_s[:, j * 384:(j + 1) * 384]), j * 384)
    rs_a(WP)
    put(PT, dot_tn(deb_s[...], oh_s[...]))
    rs_a(PT)
    low = (lax.broadcasted_iota(jnp.int32, (8, 256), 0))
    ga = gv384[...]
    gq = gvqkv[...]
    gf = gvfc[...]
    for d in range(NDEV):
        xa = pltpu.roll(ga, (D - SUB * d) % D, 1)[:, 0:256] if d else ga[:, 0:256]
        xq = pltpu.roll(gq, (QKV3 - (QKV3 // NDEV) * d) % QKV3, 1)[:, 0:256] if d else gq[:, 0:256]
        xf = pltpu.roll(gf, (FF - SUBF * d) % FF, 1)[:, 0:256] if d else gf[:, 0:256]
        tail = jnp.where(low == 2, xq, jnp.where(low == 3, xf, xa[8:16, :]))
        grads[VEC][d // 2, d % 2, 0:8, :] = xa[0:8, :]
        grads[VEC][d // 2, d % 2, 8:16, :] = tail
    rs_a(VEC)
    rs_c(QKV)
    rs_d(FC)
    rs_d(OUT)
    rs_b(WP)
    rs_b(PT)
    rs_b(VEC)

    def last(i, carry):
        rs = pl.ds(pl.multiple_of(i * TP, TP), TP)
        h1 = h_s[rs, :] + dot(gel_s[rs, :], wproj[...]) + vec('b_proj')
        h1_out[i] = h1[0:TOK, :].astype(BF16)
        return carry

    lax.fori_loop(0, IMG, last, 0)
    rs_c(WP)
    rs_c(PT)
    rs_c(VEC)
    rs_d(QKV)
    rs_d(WP)
    rs_d(PT)
    rs_d(VEC)
    for k in range(7):
        for kind in range(7):
            gcopy(k, kind).wait_send()
        for kind in range(4):
            rcopy(k, kind).wait_send()


def call_step(args):
    shapes = [(r, c) for _, r, c in MATS] + [(16, 256)]
    vm = lambda s, t: pltpu.VMEM(s, t)
    scratch = [
        vm((IMG, 128), jnp.int32), vm((NT, PX), BF16), vm((NT, PPOS), BF16),
        vm((D, PX), BF16), vm((D, PPOS), BF16), vm((D, QKV3), BF16), vm((D, D), BF16), vm((D, FF), BF16), vm((FF, D), BF16),
        vm((NDEV, 16, 256), F32), vm((16, D), F32), vm((8, QKV3), F32), vm((8, FF), F32),
        vm((NT, D), F32), vm((NT, D), F32), vm((NT, D), F32), vm((NT, 1), F32), vm((NT, 1), F32), vm((NT, 1), F32),
        vm((NT, D), F32), vm((NT, D), BF16), vm((NT, QKV3), BF16), vm((IMG * PAIRS, 2 * TP, TP), F32), vm((NT, D), BF16),
        vm((NT, D), BF16), vm((NT, FF), BF16), vm((NT, FF), BF16), vm((NT, D), BF16), vm((NT, D), F32), vm((NT, D), BF16),
        vm((NT, D), BF16), vm((NT, QKV3), BF16), vm((NT, D), BF16),
        vm((16, D), F32), vm((8, QKV3), F32), vm((8, FF), F32),
    ]
    scratch += [vm((4, 2) + s, F32) for s in shapes]
    scratch += [vm((4,) + s, F32) for s in shapes]
    scratch += [vm(s, F32) for s in shapes] * 3
    scratch += [pltpu.SemaphoreType.DMA((49,)), pltpu.SemaphoreType.DMA((49,)), pltpu.SemaphoreType.DMA((28,)), pltpu.SemaphoreType.DMA((28,))]
    vmem = pl.BlockSpec(memory_space=pltpu.VMEM)
    return pl.pallas_call(
        step_kernel,
        out_shape=[jax.ShapeDtypeStruct((IMG, TOK, D), BF16)] + [jax.ShapeDtypeStruct(s, F32) for s in shapes],
        in_specs=[vmem] * len(args),
        out_specs=[vmem] * 8,
        scratch_shapes=scratch,
        compiler_params=pltpu.CompilerParams(collective_id=0, has_side_effects=True, vmem_limit_bytes=67043328),
        name='vit_step',
    )(*args)


def solution(mesh):
    def spec_of(name):
        return P(None, AXIS) if name in LAST_SPLIT else P(AXIS)

    def local_step(patches, keep, *rest):
        w = dict(zip(PARAM_NAMES, rest[:-1]))
        args = [patches, keep, rest[-1], w['w_patch'], w['pos_table'], w['w_qkv'].reshape(SUB, QKV3), w['w_out'], w['w_fc'], w['w_proj']]
        args += [w[name].reshape(1, -1) for name in VROWS]
        h1, g_wp, g_pt, g_qkv, g_out, g_fc, g_proj, g_vec = call_step(args)
        width = {'b_qkv': QKV3 // NDEV, 'b_fc': SUBF}
        g = {name: g_vec[ROW[name], :width.get(name, SUB)] for name in VROWS}
        g['w_patch'] = g_wp.T
        g['pos_table'] = jnp.concatenate([g['cls_tok'][None], g_pt[:, 1:NPATCH + 1].T], axis=0)
        g['w_qkv'] = g_qkv.reshape(SUB, 3, 6, HD)
        g['w_out'] = g_out
        g['w_fc'] = g_fc
        g['w_proj'] = g_proj
        return (h1,) + tuple(g[name] for name in PARAM_NAMES)

    batch_spec = P(AXIS)
    param_specs = tuple(spec_of(name) for name in PARAM_NAMES)
    return jax.shard_map(local_step, mesh=mesh, in_specs=(batch_spec, batch_spec) + param_specs + (batch_spec,), out_specs=(batch_spec,) + param_specs, check_vma=False)
```
